32 devices in a mesh: rows: 8 (over y, x, core), rhs: 4 (over z).
Axes of the slice: x: 2, y: 2, z: 4, core: 2. Of those that a mesh axis runs over, the one named last changes fastest.
Arguments:
- band_blocks: float32 [64, 256, 1280], P('rows'), may hold values from -12 to 12
- precond_blocks: float32 [64, 256, 256], P('rows'), may hold values from -2 to 2
- right_side: float32 [16384, 2048], P('rows', 'rhs'), may hold values from -80 to 80
Outputs:
- solution: float32 [16384, 2048], P('rows', 'rhs')
- scaled_residual: float32 [16384, 2048], P('rows', 'rhs')
- rms_history: float32 [3, 2048], P(None, 'rhs')
- overall_rms: float32 [], replicated
The draws below stay inside these ranges and needn't reach their ends.
All inputs are finite; a program needn't handle non-finite values.
Results may differ from the reference program's by a relative error of at most 0.0003.
Values sent between devices are 32-bit elements; how exact they have to be, the bound alone decides.
No kernel may reach another device: no remote copies, remote signals or barrier semaphores. Data moves between devices by JAX's collectives and lax.ppermute only.
A program may use at most 128 MiB of HBM per device.

```python
import math
import jax
import jax.numpy as jnp
from jax import lax

B = 256
ITERS = 2
NBLOCKS = 64
N = 16384
NRHS = 2048


def band_parts(key):
    base = jax.random.fold_in(key, 1234)
    key_scale, key_inner, key_outer = jax.random.split(base, 3)
    scales = jnp.exp(jax.random.uniform(key_scale, (NBLOCKS,), jnp.float32) * math.log(10.0))
    inner = jax.random.normal(key_inner, (NBLOCKS, B, B), jnp.float32) * (0.15 / math.sqrt(B))
    outer = jax.random.normal(key_outer, (NBLOCKS, B, 4 * B), jnp.float32) * (0.15 / math.sqrt(B))
    return (scales, inner, outer)


def draw_band_blocks(key, part):
    scales, inner, outer = band_parts(key)
    identity = jnp.eye(B, dtype=jnp.float32)
    center = scales[:, None, None] * (identity[None, :, :] + inner)
    pieces = []
    for number, offset in enumerate([-2, -1, 1, 2]):
        beside = jnp.roll(scales, -offset)
        pieces.append(outer[:, :, number * B:(number + 1) * B] * jnp.sqrt(scales * beside)[:, None, None])
    return jnp.concatenate([pieces[0], pieces[1], center, pieces[2], pieces[3]], axis=2)


def draw_precond_blocks(key, part):
    scales, inner, outer = band_parts(key)
    identity = jnp.eye(B, dtype=jnp.float32)
    square = jnp.einsum('jab,jbc->jac', inner, inner, precision=lax.Precision.HIGHEST)
    return (identity[None, :, :] - inner + square) / scales[:, None, None]


def draw_right_side(key, part):
    base = jax.random.fold_in(key, 77)
    key_value, key_column = jax.random.split(base, 2)
    row_frac = jnp.arange(N, dtype=jnp.float32) / N
    row_scale = jnp.exp(row_frac * math.log(10.0)) / math.sqrt(10.0)
    column_frac = jnp.arange(NRHS, dtype=jnp.float32) / NRHS
    column_scale = jnp.exp(column_frac * math.log(3.0)) * (1.0 + jax.random.uniform(key_column, (NRHS,), jnp.float32))
    values = jnp.clip(jax.random.normal(key_value, (N, NRHS), jnp.float32), -4.0, 4.0)
    return values * row_scale[:, None] * column_scale[None, :]


def setup_inputs(seed: int = 0) -> dict:
    seeds = jax.random.split(jax.random.key(seed), 4)
    return {
        "band_blocks": draw_band_blocks(jax.random.fold_in(seeds[3], 71), 0),
        "precond_blocks": draw_precond_blocks(jax.random.fold_in(seeds[3], 71), 0),
        "right_side": draw_right_side(jax.random.fold_in(seeds[3], 71), 0),
    }


def band_times(band_blocks, operand):
    padded = jnp.pad(operand, ((2 * B, 2 * B), (0, 0)))
    indices = jnp.arange(NBLOCKS, dtype=jnp.int32)

    def one_block(pair):
        block, index = pair
        window = lax.dynamic_slice_in_dim(padded, (index * B).astype(jnp.int32), 5 * B, 0)
        return jnp.dot(block, window, precision=lax.Precision.HIGHEST, preferred_element_type=jnp.float32)
    return lax.map(one_block, (band_blocks, indices)).reshape(operand.shape[0], operand.shape[1])

def precondition(precond_blocks, operand):
    shaped = operand.reshape(NBLOCKS, B, operand.shape[1])
    return jnp.einsum('jab,jbc->jac', precond_blocks, shaped, precision=lax.Precision.HIGHEST).reshape(operand.shape)

def reference(band_blocks, precond_blocks, right_side):
    solution = precondition(precond_blocks, right_side)
    sums = []
    residual = right_side
    for sweep in range(ITERS + 1):
        residual = right_side - band_times(band_blocks, solution)
        sums.append(lax.optimization_barrier(jnp.sum(residual * residual, axis=0)))
        if sweep < ITERS:
            solution = solution + precondition(precond_blocks, residual)
    stacked = jnp.stack(sums)
    history = jnp.sqrt(stacked / N + 1e-06)
    scaled_residual = residual / history[ITERS][None, :]
    overall_rms = jnp.sqrt(jnp.sum(stacked[ITERS]) / (N * NRHS) + 1e-06)
    return (solution, scaled_residual, history, overall_rms)
```

```python
import jax
import jax.numpy as jnp
from jax import lax
from jax.experimental import pallas as pl
from jax.experimental.pallas import tpu as pltpu
from jax.sharding import PartitionSpec as P

ITERS = 2
REACH = 2
EPS = 1e-06
CHUNKS = 2
LIMIT = 12 * 2**20


def split(value):
    high = value.astype(jnp.bfloat16)
    low = (value - high.astype(jnp.float32)).astype(jnp.bfloat16)
    return high, low


def dot3(left_high, left_low, right_high, right_low):
    def dot(left, right):
        return jnp.dot(left, right, preferred_element_type=jnp.float32)

    return dot(left_high, right_high) + (dot(left_high, right_low) + dot(left_low, right_high))


def whole():
    return pl.BlockSpec(memory_space=pltpu.VMEM)


def scalar():
    return pl.BlockSpec(memory_space=pltpu.SMEM)


def call(kernel, name, out_shapes, in_specs, out_specs, flops, args, grid=(), scratch=(), aliases=None):
    return pl.pallas_call(
        kernel,
        name=name,
        grid=grid,
        in_specs=in_specs,
        out_specs=out_specs,
        out_shape=out_shapes,
        scratch_shapes=scratch,
        input_output_aliases=aliases or {},
        compiler_params=pltpu.CompilerParams(vmem_limit_bytes=LIMIT),
        cost_estimate=pl.CostEstimate(flops=flops, bytes_accessed=0, transcendentals=0),
    )(*args)


def f32(*shape):
    return jax.ShapeDtypeStruct(shape, jnp.float32)


def bf16(*shape):
    return jax.ShapeDtypeStruct(shape, jnp.bfloat16)


def in_hbm(value):
    return pltpu.with_memory_space_constraint(value, pltpu.HBM)


def store_sends(odd_ref, edge_ref, cross_ref, core_ref):
    half = edge_ref.shape[0] // 2
    first = odd_ref[0] * half
    first = pl.multiple_of(first, 256) if half % 256 == 0 else first
    second = half - first
    second = pl.multiple_of(second, 256) if half % 256 == 0 else second
    cross_ref[...] = edge_ref[pl.ds(first, half), :]
    core_ref[...] = edge_ref[pl.ds(second, half), :]


def prepare_kernel(value_ref, high_ref, low_ref):
    high, low = split(value_ref[...])
    high_ref[...] = high
    low_ref[...] = low


def prepare(value):
    count, rows, width = value.shape
    spec = pl.BlockSpec((1, rows, width), lambda i: (i, 0, 0))
    return call(
        prepare_kernel, "prepare", (bf16(*value.shape), bf16(*value.shape)), [spec], (spec, spec),
        value.size, (value,), grid=(count,),
    )


def first_edges(right_side, precond, odd, chunk, width, after):
    nb, br, _ = precond.shape
    edge = REACH * br
    rows = nb * br

    def kernel(odd_ref, right_ref, matrix_ref, *refs):
        edge_ref, cross_ref, core_ref, value, matrix, arrived = refs[-6:]
        columns = pl.ds(chunk * width, width)
        copies = []
        for side, (row, block) in enumerate(((0, 0), (rows - edge, nb - REACH))):
            copies.append(
                (
                    pltpu.make_async_copy(
                        right_ref.at[pl.ds(row, edge), columns], value.at[side], arrived.at[2 * side]
                    ),
                    pltpu.make_async_copy(
                        matrix_ref.at[pl.ds(block, REACH)], matrix.at[side], arrived.at[2 * side + 1]
                    ),
                )
            )
        for pair in copies:
            for copy in pair:
                copy.start()
        for side, pair in enumerate(copies):
            for copy in pair:
                copy.wait()
            for j in range(REACH):
                here = split(matrix[side, j])
                data = split(value[side, j * br : (j + 1) * br, :])
                edge_ref[side * edge + j * br : side * edge + (j + 1) * br, :] = dot3(*here, *data)
        store_sends(odd_ref, edge_ref, cross_ref, core_ref)

    args = [odd, in_hbm(right_side), in_hbm(precond)]
    specs = [scalar()] + [pl.BlockSpec(memory_space=pltpu.HBM)] * 2
    if after is not None:
        args.append(after)
        specs.append(pl.BlockSpec(memory_space=pl.ANY))
    return call(
        kernel, "first_edges",
        (f32(2 * edge, width), f32(edge, width), f32(edge, width)),
        specs,
        (whole(), whole(), whole()),
        6 * 2 * REACH * br * br * width,
        args,
        scratch=[
            pltpu.VMEM((2, edge, width), jnp.float32),
            pltpu.VMEM((2, REACH, br, br), jnp.float32),
            pltpu.SemaphoreType.DMA((4,)),
        ],
    )


def bulk(residual, edge_step, total, band, precond, nb, br, width, chunk, out_width, into, after=None):
    first = total is None
    final = into is not None
    edge = REACH * br
    rows = nb * br
    inner = rows - 2 * edge
    reach = 2 * REACH + 1

    def kernel(*refs):
        refs = list(refs)
        if first:
            right_ref = refs.pop(0)
            edge_of = lambda j: right_ref.at[pl.ds(j * br, br), :]
            inner_of = edge_of
        else:
            redge_ref, rinner_ref = refs.pop(0), refs.pop(0)
        dedge_ref = refs.pop(0)
        if not first:
            total_ref = refs.pop(0)
        ah_ref, al_ref, mh_ref, ml_ref = [refs.pop(0) for _ in range(4)]
        if final and into is not True:
            refs.pop(0)
        if after is not None:
            refs.pop(0)
        outedge_ref, outinner_ref, outtotal_ref = [refs.pop(0) for _ in range(3)]
        if not first:
            squares_ref = refs.pop(0)
        dh_ref, dl_ref = refs

        def rows_of(j):
            if first:
                return right_ref[pl.ds(pl.multiple_of(j * br, br), br), :]
            return rinner_ref[pl.ds(pl.multiple_of((j - REACH) * br, br), br), :]

        def edge_rows(j):
            if first:
                return right_ref[j * br : (j + 1) * br, :]
            k = j if j < REACH else j - nb + 2 * REACH
            return redge_ref[k * br : (k + 1) * br, :]

        for j in list(range(REACH)) + list(range(nb - REACH, nb)):
            k = j if j < REACH else j - nb + 2 * REACH
            d = dedge_ref[k * br : (k + 1) * br, :]
            high, low = split(d)
            dh_ref[j * br : (j + 1) * br, :] = high
            dl_ref[j * br : (j + 1) * br, :] = low
            if first:
                outtotal_ref[j * br : (j + 1) * br, :] = d
            else:
                outtotal_ref[j * br : (j + 1) * br, :] = total_ref[j * br : (j + 1) * br, :] + d

        def make(j):
            value = rows_of(j)
            d = dot3(mh_ref[j], ml_ref[j], *split(value))
            high, low = split(d)
            here = pl.ds(pl.multiple_of(j * br, br), br)
            dh_ref[here, :] = high
            dl_ref[here, :] = low
            if first:
                outtotal_ref[here, :] = d
            else:
                outtotal_ref[here, :] = total_ref[here, :] + d

        for j in range(REACH, nb - REACH):
            make(j)

        if not first:
            squares = jnp.zeros((8, width), jnp.float32)
            for j in range(nb):
                value = edge_rows(j) if j < REACH or j >= nb - REACH else rows_of(j)
                squares = squares + jnp.sum((value * value).reshape(-1, 8, width), axis=0)
            squares_ref[...] = jnp.sum(squares, axis=0, keepdims=True)

        for j in range(nb):
            start, stop = max(0, REACH - j), min(reach, nb + REACH - j)
            here = pl.ds((j + start - REACH) * br, (stop - start) * br)
            columns = slice(start * br, stop * br)
            product = dot3(ah_ref[j, :, columns], al_ref[j, :, columns], dh_ref[here, :], dl_ref[here, :])
            if j < REACH or j >= nb - REACH:
                k = j if j < REACH else j - nb + 2 * REACH
                outedge_ref[k * br : (k + 1) * br, :] = edge_rows(j) - product
            else:
                outinner_ref[(j - REACH) * br : (j - REACH + 1) * br, :] = rows_of(j) - product

    one = (1,)
    full = lambda shape: pl.BlockSpec(shape, lambda i: (0,) * len(shape))
    if first:
        specs = [pl.BlockSpec((rows, width), lambda i: (0, chunk))]
    else:
        specs = [whole(), whole()]
    specs += [whole()]
    if not first:
        specs += [whole()]
    args = [*residual, edge_step] + ([] if first else [total]) + [*band, *precond]
    specs += [whole()] * 4
    aliases = {}
    total_shape = f32(rows, width)
    total_spec = whole()
    if final:
        total_shape = f32(rows, out_width)
        total_spec = pl.BlockSpec((rows, width), lambda i: (0, chunk))
        if into is not True:
            aliases = {len(args): 2}
            args.append(into)
            specs.append(pl.BlockSpec(memory_space=pl.ANY))
    if after is not None:
        args.append(after)
        specs.append(pl.BlockSpec(memory_space=pl.ANY))
    shapes = [f32(2 * edge, width), f32(inner, width), total_shape]
    outs = [whole(), whole(), total_spec]
    if not first:
        shapes.append(f32(1, width))
        outs.append(whole())
    products = (nb - 2 * REACH) + nb * reach - REACH * (REACH + 1)
    return call(
        kernel, "bulk", tuple(shapes), specs, tuple(outs), 6 * products * br * br * width, args, grid=one,
        scratch=[pltpu.VMEM((rows, width), jnp.bfloat16), pltpu.VMEM((rows, width), jnp.bfloat16)],
        aliases=aliases,
    )


def edges(partial_edge, cross, core, band, precond, odd, nb, br, width, after, last=None):
    edge = REACH * br

    def kernel(*refs):
        refs = list(refs)
        odd_ref, part_ref, cross_ref, core_ref, ah_ref, al_ref = [refs.pop(0) for _ in range(6)]
        if last is None:
            mh_ref, ml_ref = refs.pop(0), refs.pop(0)
        else:
            inner_ref = refs.pop(0)
            known = [refs.pop(0) for _ in last[1]]
        refs.pop(0)
        if last is None:
            out_ref, step_ref, sendx_ref, sends_ref, hh_ref, hl_ref = refs
        else:
            out_ref, message_ref, hh_ref, hl_ref = refs
        odd_value = odd_ref[0]
        for ref, slot in ((cross_ref, odd_value), (core_ref, 1 - odd_value)):
            high, low = split(ref[...])
            hh_ref[pl.ds(pl.multiple_of(slot * edge, 8), edge), :] = high
            hl_ref[pl.ds(pl.multiple_of(slot * edge, 8), edge), :] = low
        squares = jnp.zeros((8, width), jnp.float32)
        for k in range(2 * REACH):
            j = k if k < REACH else k + nb - 2 * REACH
            if k < REACH:
                columns = slice(0, (REACH - k) * br)
                here = slice(k * br, edge)
            else:
                reached = k - REACH + 1
                columns = slice((2 * REACH + 1 - reached) * br, (2 * REACH + 1) * br)
                here = slice(edge, edge + reached * br)
            product = dot3(ah_ref[j, :, columns], al_ref[j, :, columns], hh_ref[here, :], hl_ref[here, :])
            value = part_ref[k * br : (k + 1) * br, :] - product
            out_ref[k * br : (k + 1) * br, :] = value
            if last is not None:
                squares = squares + jnp.sum((value * value).reshape(-1, 8, width), axis=0)
            else:
                step_ref[k * br : (k + 1) * br, :] = dot3(mh_ref[j], ml_ref[j], *split(value))
        if last is not None:
            for j in range(nb - 2 * REACH):
                value = inner_ref[j * br : (j + 1) * br, :]
                squares = squares + jnp.sum((value * value).reshape(-1, 8, width), axis=0)
            own = jnp.sum(squares, axis=0, keepdims=True)
            if not known:
                message_ref[...] = own
            for k, piece in enumerate([ref[...] for ref in known] + [own] if known else []):
                shape = (message_ref.shape[0], 1, width)
                message_ref[:, :, k * width : (k + 1) * width] = jnp.broadcast_to(piece[None], shape)
        else:
            store_sends(odd_ref, step_ref, sendx_ref, sends_ref)

    products = REACH * (REACH + 1) + (2 * REACH if last is None else 0)
    args = [odd, partial_edge, cross, core, *band]
    if last is not None:
        devices, known_sums, inner_rows = last[0], last[1], last[2]
        args += [inner_rows, *known_sums]
        sent = f32(devices, 1, (1 + len(known_sums)) * width) if known_sums else f32(1, width)
        shapes = (f32(2 * edge, width), sent)
    else:
        args += [*precond]
        shapes = (f32(2 * edge, width), f32(2 * edge, width), f32(edge, width), f32(edge, width))
    specs = [scalar()] + [whole()] * (len(args) - 1) + [pl.BlockSpec(memory_space=pl.ANY)]
    args.append(after)
    return call(
        kernel, "edges" if last is None else "edges_last", shapes, specs,
        tuple(whole() for _ in shapes), 6 * products * br * br * width, args,
        scratch=[pltpu.VMEM((2 * edge, width), jnp.bfloat16), pltpu.VMEM((2 * edge, width), jnp.bfloat16)],
    )


def scale_out(state, gathered, place, count, across, nb, br, width):
    rows = nb * br
    edge = REACH * br
    inner_steps = (nb - 2 * REACH) // REACH
    steps = inner_steps + 2
    part = width // CHUNKS
    total_rows = count * rows

    def kernel(place_ref, *refs):
        pieces = refs[: 2 * CHUNKS]
        here_ref, out_ref, history_ref, overall_ref, inverse_ref = refs[2 * CHUNKS :]
        step = pl.program_id(0)

        @pl.when(step == 0)
        def _():
            place_value = place_ref[0]
            for sweep in range(ITERS + 1):
                columns = slice(sweep * width, (sweep + 1) * width)
                value = here_ref[place_value, :, columns]
                for row in range(1, count):
                    value = value + here_ref[place_value + row * across, :, columns]
                root = jnp.sqrt(value / total_rows + EPS)
                history_ref[sweep : sweep + 1, :] = root
            inverse_ref[...] = 1.0 / root
            everything = jnp.sum(here_ref[:, :, ITERS * width :], axis=0)
            total = jnp.sum(everything, axis=1, keepdims=True)
            overall_ref[...] = jnp.sqrt(total / (total_rows * across * width) + EPS)

        def write(inner):
            for c in range(CHUNKS):
                columns = slice(c * part, (c + 1) * part)
                ref = pieces[2 * c + (1 if inner else 0)]
                out_ref[:, columns] = ref[...] * inverse_ref[:, columns]

        inside = (step > 0) & (step < steps - 1)
        pl.when(inside)(lambda: write(True))
        pl.when(jnp.logical_not(inside))(lambda: write(False))

    args, specs = [place], [scalar()]
    for outer, inner in state:
        args += [outer, inner]
        specs += [
            pl.BlockSpec((edge, part), lambda i: (i // (steps - 1), 0)),
            pl.BlockSpec((edge, part), lambda i: (jnp.clip(i - 1, 0, inner_steps - 1), 0)),
        ]
    return call(
        kernel, "scale_out", (f32(rows, width), f32(ITERS + 1, width), f32(1, 1)), specs + [whole()],
        (pl.BlockSpec((edge, width), lambda i: (i, 0)), whole(), whole()),
        rows * width, args + [gathered], grid=(steps,),
        scratch=[pltpu.VMEM((1, width), jnp.float32)],
    )


def swaps(count):
    core = [(i, i ^ 1) for i in range(count) if (i ^ 1) < count]
    cross = []
    for i in range(1, count - 1, 2):
        cross += [(i, i + 1), (i + 1, i)]
    return core, cross


def shards(band_blocks, precond_blocks, right_side):
    nb, br, _ = precond_blocks.shape
    width = right_side.shape[1]
    part = width // CHUNKS
    count = lax.axis_size("rows")
    across = lax.axis_size("rhs")
    core_pairs, cross_pairs = swaps(count)
    odd = (lax.axis_index("rows") % 2).astype(jnp.int32)[None]

    def exchange(cross_send, core_send):
        return lax.ppermute(cross_send, "rows", cross_pairs), lax.ppermute(core_send, "rows", core_pairs)

    place = lax.axis_index("rhs").astype(jnp.int32)[None]
    step, halo = [], []
    for c in range(CHUNKS):
        edge_step, cross_send, core_send = first_edges(
            right_side, precond_blocks, odd, c, part, step[-1] if c else None
        )
        step.append(edge_step)
        halo.append(exchange(cross_send, core_send))
    band = prepare(band_blocks)
    precond = prepare(precond_blocks)
    state = [None] * CHUNKS
    sums = [[None] * CHUNKS for _ in range(ITERS)]
    total = [None] * CHUNKS
    answer, after = None, step[-1]
    for c in range(CHUNKS):
        outer, inner, total[c] = bulk(
            (right_side,), step[c], None, band, precond, nb, br, part, c, width, None, after
        )
        state[c] = (outer, inner)
        after = outer
    for sweep in range(ITERS):
        for c in range(CHUNKS):
            outer, inner = state[c]
            outer, step[c], cross_send, core_send = edges(
                outer, *halo[c], band, precond, odd, nb, br, part, after
            )
            halo[c] = exchange(cross_send, core_send)
            into = None
            if sweep == ITERS - 1:
                into = True if answer is None else answer
            outer, inner, total[c], sums[sweep][c] = bulk(
                (outer, inner), step[c], total[c], band, precond, nb, br, part, c, width, into
            )
            if into is not None:
                answer = total[c]
            after = outer
            state[c] = (outer, inner)
    known = [s for row in sums for s in row]
    for c in range(CHUNKS):
        outer, inner = state[c]
        send = known if c == CHUNKS - 1 else []
        outer, message = edges(
            outer, *halo[c], band, precond, odd, nb, br, part, after, (count * across, send, inner)
        )
        known.append(message)
        after = outer
        state[c] = (outer, inner)
    gathered = lax.all_to_all(message, ("rows", "rhs"), 0, 0, tiled=True)
    scaled, history, overall = scale_out(state, gathered, place, count, across, nb, br, width)
    return (answer, scaled, history, overall.reshape(()))


def solution(mesh):
    in_specs = (P("rows", None, None), P("rows", None, None), P("rows", "rhs"))
    out_specs = (P("rows", "rhs"), P("rows", "rhs"), P(None, "rhs"), P())
    return jax.shard_map(shards, mesh=mesh, in_specs=in_specs, out_specs=out_specs, check_vma=False)
```

```python
import jax
import jax.numpy as jnp
from jax import lax
from jax.experimental import pallas as pl
from jax.experimental.pallas import tpu as pltpu
from jax.sharding import PartitionSpec as P


ITERS = 2
REACH = 2
EPS = 1e-06
CHUNKS = 2
LANES = 128
LIMIT = 12 * 2**20


def split(value):
    high = value.astype(jnp.bfloat16)
    low = (value - high.astype(jnp.float32)).astype(jnp.bfloat16)
    return high, low


def dot3(left_high, left_low, right_high, right_low):
    def dot(left, right):
        return jnp.dot(left, right, preferred_element_type=jnp.float32)

    return dot(left_high, right_high) + (dot(left_high, right_low) + dot(left_low, right_high))


def whole():
    return pl.BlockSpec(memory_space=pltpu.VMEM)


def scalar():
    return pl.BlockSpec(memory_space=pltpu.SMEM)


def call(kernel, out_shapes, in_specs, out_specs, flops, args, grid=(), scratch=(), aliases=None):
    return pl.pallas_call(
        kernel,
        grid=grid,
        in_specs=in_specs,
        out_specs=out_specs,
        out_shape=out_shapes,
        scratch_shapes=scratch,
        input_output_aliases=aliases or {},
        compiler_params=pltpu.CompilerParams(vmem_limit_bytes=LIMIT),
        cost_estimate=pl.CostEstimate(flops=flops, bytes_accessed=0, transcendentals=0),
    )(*args)


def f32(*shape):
    return jax.ShapeDtypeStruct(shape, jnp.float32)


def bf16(*shape):
    return jax.ShapeDtypeStruct(shape, jnp.bfloat16)


def in_hbm(value):
    return pltpu.with_memory_space_constraint(value, pltpu.HBM)


def store_sends(odd_ref, edge_ref, cross_ref, core_ref):
    half = edge_ref.shape[0] // 2
    first = odd_ref[0] * half
    first = pl.multiple_of(first, 256) if half % 256 == 0 else first
    second = half - first
    second = pl.multiple_of(second, 256) if half % 256 == 0 else second
    cross_ref[...] = edge_ref[pl.ds(first, half), :]
    core_ref[...] = edge_ref[pl.ds(second, half), :]


def prepare_kernel(value_ref, high_ref, low_ref):
    high, low = split(value_ref[...])
    high_ref[...] = high
    low_ref[...] = low


def prepare(value):
    count, rows, width = value.shape
    spec = pl.BlockSpec((1, rows, width), lambda i: (i, 0, 0))
    return call(
        prepare_kernel, (bf16(*value.shape), bf16(*value.shape)), [spec], (spec, spec),
        value.size, (value,), grid=(count,),
    )


def first_edges(right_side, precond, odd, across, chunk, width, after):
    nb, br, _ = precond.shape
    edge = REACH * br
    rows = nb * br

    def kernel(odd_ref, right_ref, matrix_ref, *refs):
        out_ref, value, matrix, arrived = refs[-4:]
        above = odd_ref[0] if across else 1 - odd_ref[0]
        here = pl.ds(pl.multiple_of(above * (rows - edge), edge), edge)
        copies = [
            pltpu.make_async_copy(right_ref.at[here, pl.ds(chunk * width, width)], value, arrived.at[0]),
            pltpu.make_async_copy(matrix_ref.at[pl.ds(above * (nb - REACH), REACH)], matrix, arrived.at[1]),
        ]
        for copy in copies:
            copy.start()
        for copy in copies:
            copy.wait()
        for j in range(REACH):
            data = split(value[j * br : (j + 1) * br, :])
            out_ref[j * br : (j + 1) * br, :] = dot3(*split(matrix[j]), *data)

    args = [odd, in_hbm(right_side), in_hbm(precond)]
    specs = [scalar()] + [pl.BlockSpec(memory_space=pltpu.HBM)] * 2
    if after is not None:
        args.append(after)
        specs.append(pl.BlockSpec(memory_space=pl.ANY))
    return call(
        kernel, f32(edge, width), specs, whole(), 6 * REACH * br * br * width, args,
        scratch=[
            pltpu.VMEM((edge, width), jnp.float32),
            pltpu.VMEM((REACH, br, br), jnp.float32),
            pltpu.SemaphoreType.DMA((2,)),
        ],
    )


def other_edges(right_side, precond, odd, width, after):
    nb, br, _ = precond.shape
    edge = REACH * br
    rows = nb * br
    todo = [(c, across) for c in range(CHUNKS) for across in (True, False)][1:]

    def kernel(odd_ref, right_ref, matrix_ref, _, *out_refs):
        for (c, across), out_ref in zip(todo, out_refs):
            above = odd_ref[0] if across else 1 - odd_ref[0]
            base = pl.multiple_of(above * (rows - edge), edge)
            for j in range(REACH):
                data = split(right_ref[pl.ds(base + j * br, br), c * width : (c + 1) * width])
                matrix = split(matrix_ref[above * (nb - REACH) + j])
                out_ref[j * br : (j + 1) * br, :] = dot3(*matrix, *data)

    return call(
        kernel, tuple(f32(edge, width) for _ in todo),
        [scalar(), whole(), whole(), pl.BlockSpec(memory_space=pl.ANY)], tuple(whole() for _ in todo),
        6 * REACH * len(todo) * br * br * width, [odd, right_side, precond, after],
    )


def bulk(residual, edge_step, total, band, precond, nb, br, width, chunk, after):
    first = total is None
    edge = REACH * br
    rows = nb * br
    inner = rows - 2 * edge
    reach = 2 * REACH + 1
    edge_rows = [*range(REACH), *range(nb - REACH, nb)]

    def at(j):
        return slice(j * br, (j + 1) * br)

    def kernel(*refs):
        refs = list(refs)
        if first:
            right_ref, odd_ref, cross_ref, core_ref = [refs.pop(0) for _ in range(4)]
        else:
            redge_ref, rinner_ref, dedge_ref, total_ref = [refs.pop(0) for _ in range(4)]
        ah_ref, al_ref, mh_ref, ml_ref, _, outedge_ref, outinner_ref, outtotal_ref = [refs.pop(0) for _ in range(8)]
        if not first:
            squares_ref = refs.pop(0)
        dh_ref, dl_ref = refs

        def load(j):
            if first:
                return right_ref[at(j), :]
            if j in edge_rows:
                return redge_ref[at(edge_rows.index(j)), :]
            return rinner_ref[at(j - REACH), :]

        def keep(j, d):
            high, low = split(d)
            dh_ref[at(j), :] = high
            dl_ref[at(j), :] = low
            outtotal_ref[at(j), :] = d if first else total_ref[at(j), :] + d

        if first:
            for ref, above in ((cross_ref, odd_ref[0]), (core_ref, 1 - odd_ref[0])):
                high, low = split(ref[...])
                here = pl.ds(pl.multiple_of(above * (rows - edge), edge), edge)
                dh_ref[here, :] = high
                dl_ref[here, :] = low
                outtotal_ref[here, :] = ref[...]
        else:
            for k, j in enumerate(edge_rows):
                keep(j, dedge_ref[at(k), :])
        for j in range(REACH, nb - REACH):
            keep(j, dot3(mh_ref[j], ml_ref[j], *split(load(j))))
        if not first:
            squares = jnp.zeros((8, width), jnp.float32)
            for j in range(nb):
                value = load(j)
                squares = squares + jnp.sum((value * value).reshape(-1, 8, width), axis=0)
            squares_ref[...] = jnp.sum(squares, axis=0, keepdims=True)
        for j in range(nb):
            start, stop = max(0, REACH - j), min(reach, nb + REACH - j)
            here = slice((j + start - REACH) * br, (j + stop - REACH) * br)
            columns = slice(start * br, stop * br)
            product = dot3(ah_ref[j, :, columns], al_ref[j, :, columns], dh_ref[here, :], dl_ref[here, :])
            if j in edge_rows:
                outedge_ref[at(edge_rows.index(j)), :] = load(j) - product
            else:
                outinner_ref[at(j - REACH), :] = load(j) - product

    specs = [pl.BlockSpec((rows, width), lambda i: (0, chunk)), scalar()] if first else [whole(), whole()]
    args = [*residual, *edge_step] + ([] if first else [total]) + [*band, *precond, after]
    specs += [whole()] * (len(args) - len(specs) - 1) + [pl.BlockSpec(memory_space=pl.ANY)]
    shapes = [f32(2 * edge, width), f32(inner, width), f32(rows, width)] + ([] if first else [f32(1, width)])
    products = (nb - 2 * REACH) + nb * reach - REACH * (REACH + 1)
    return call(
        kernel, tuple(shapes), specs, tuple(whole() for _ in shapes), 6 * products * br * br * width, args,
        grid=(1,), scratch=[pltpu.VMEM((rows, width), jnp.bfloat16), pltpu.VMEM((rows, width), jnp.bfloat16)],
    )


def halo_products(odd_ref, cross_ref, core_ref, ah_ref, al_ref, hh_ref, hl_ref, nb, br):
    edge = REACH * br
    odd_value = odd_ref[0]
    for ref, slot in ((cross_ref, odd_value), (core_ref, 1 - odd_value)):
        high, low = split(ref[...])
        here = pl.ds(pl.multiple_of(slot * edge, 8), edge)
        hh_ref[here, :] = high
        hl_ref[here, :] = low

    def product(k):
        if k < REACH:
            j, columns, here = k, slice(0, (REACH - k) * br), slice(k * br, edge)
        else:
            reached = k - REACH + 1
            j = k + nb - 2 * REACH
            columns = slice((2 * REACH + 1 - reached) * br, (2 * REACH + 1) * br)
            here = slice(edge, edge + reached * br)
        return dot3(ah_ref[j, :, columns], al_ref[j, :, columns], hh_ref[here, :], hl_ref[here, :])

    return product


def edges(partial_edge, cross, core, band, precond, odd, nb, br, width, after):
    edge = REACH * br

    def kernel(odd_ref, part_ref, cross_ref, core_ref, ah_ref, al_ref, mh_ref, ml_ref, _, *refs):
        out_ref, step_ref, sendx_ref, sends_ref, hh_ref, hl_ref = refs
        product = halo_products(odd_ref, cross_ref, core_ref, ah_ref, al_ref, hh_ref, hl_ref, nb, br)
        for k in range(2 * REACH):
            j = k if k < REACH else k + nb - 2 * REACH
            value = part_ref[k * br : (k + 1) * br, :] - product(k)
            out_ref[k * br : (k + 1) * br, :] = value
            step_ref[k * br : (k + 1) * br, :] = dot3(mh_ref[j], ml_ref[j], *split(value))
        store_sends(odd_ref, step_ref, sendx_ref, sends_ref)

    shapes = (f32(2 * edge, width), f32(2 * edge, width), f32(edge, width), f32(edge, width))
    args = [odd, partial_edge, cross, core, *band, *precond, after]
    specs = [scalar()] + [whole()] * (len(args) - 2) + [pl.BlockSpec(memory_space=pl.ANY)]
    return call(
        kernel, shapes, specs, tuple(whole() for _ in shapes),
        6 * (REACH * (REACH + 1) + 2 * REACH) * br * br * width, args,
        scratch=[pltpu.VMEM((2 * edge, width), jnp.bfloat16), pltpu.VMEM((2 * edge, width), jnp.bfloat16)],
    )


def edges_last(partial_edge, inner, cross, core, band, odd, nb, br, width, after, totals, earlier, devices):
    edge = REACH * br
    rows = nb * br
    answering = totals is not None

    def kernel(odd_ref, part_ref, inner_ref, cross_ref, core_ref, ah_ref, al_ref, *refs):
        refs = list(refs)
        copies = []
        if answering:
            total_refs = [refs.pop(0) for _ in range(CHUNKS)]
            _, out_ref, sums_ref, answer_ref, hh_ref, hl_ref, answered = refs
            for c in range(CHUNKS):
                there = answer_ref.at[:, pl.ds(c * width, width)]
                copies.append(pltpu.make_async_copy(total_refs[c], there, answered.at[c]))
                copies[-1].start()
        else:
            earlier_ref, _, out_ref, sums_ref, hh_ref, hl_ref = refs
        product = halo_products(odd_ref, cross_ref, core_ref, ah_ref, al_ref, hh_ref, hl_ref, nb, br)
        squares = jnp.zeros((8, width), jnp.float32)
        for k in range(2 * REACH):
            here = pl.ds(k * br, br)
            value = part_ref[here, :] - product(k)
            out_ref[here, :] = value
            squares = squares + jnp.sum((value * value).reshape(-1, 8, width), axis=0)
        for j in range(nb - 2 * REACH):
            value = inner_ref[j * br : (j + 1) * br, :]
            squares = squares + jnp.sum((value * value).reshape(-1, 8, width), axis=0)
        own = jnp.sum(squares, axis=0, keepdims=True)
        if answering:
            sums_ref[...] = own
        else:
            sums_ref[:, :, :width] = jnp.broadcast_to(own[None], (devices, 1, width))
            folded = earlier_ref[:, :LANES]
            for k in range(1, earlier_ref.shape[1] // LANES):
                folded = folded + earlier_ref[:, k * LANES : (k + 1) * LANES]
            sums_ref[:, :, width:] = jnp.broadcast_to(folded[None], (devices, 1, LANES))
        for copy in copies:
            copy.wait()

    args = [odd, partial_edge, inner, cross, core, *band]
    args += [*totals] if answering else [earlier]
    specs = [scalar()] + [whole()] * (len(args) - 1) + [pl.BlockSpec(memory_space=pl.ANY)]
    args.append(after)
    hbm = pl.BlockSpec(memory_space=pltpu.HBM)
    shapes = [f32(2 * edge, width)]
    shapes += [f32(1, width), pltpu.HBM((rows, CHUNKS * width), jnp.float32)] if answering else [f32(devices, 1, width + LANES)]
    outs = [whole(), whole()] + ([hbm] if answering else [])
    scratch = [
        pltpu.VMEM((2 * edge, width), jnp.bfloat16),
        pltpu.VMEM((2 * edge, width), jnp.bfloat16),
    ] + ([pltpu.SemaphoreType.DMA((CHUNKS,))] if answering else [])
    return call(
        kernel, tuple(shapes), specs, tuple(outs), 6 * REACH * (REACH + 1) * br * br * width, args,
        scratch=scratch,
    )


def scale_out(state, gathered, known, place, count, across, nb, br, width):
    rows = nb * br
    edge = REACH * br
    part = width // CHUNKS
    total_rows = count * rows

    def kernel(place_ref, *refs):
        pieces = refs[: 2 * CHUNKS]
        here_ref, known_ref, out_ref, history_ref, overall_ref, away, scaled, inverse, fetched, stored = refs[2 * CHUNKS :]
        fetch = pltpu.make_async_copy(pieces[1], away, fetched.at[0])
        fetch.start()
        place_value = place_ref[0]
        sums = [known_ref[:, k * part : (k + 1) * part] for k in range(known_ref.shape[1] // part)]
        value = here_ref[place_value, :, :part]
        for row in range(1, count):
            value = value + here_ref[place_value + row * across, :, :part]
        for k, value in enumerate(sums + [value]):
            sweep, c = divmod(k, CHUNKS)
            columns = slice(c * part, (c + 1) * part)
            root = jnp.sqrt(value / total_rows + EPS)
            history_ref[sweep : sweep + 1, columns] = root
            if sweep == ITERS:
                inverse[:, columns] = 1.0 / root
        copies = []
        jobs = [(c, 0, 0) for c in range(CHUNKS)] + [(c, 0, edge) for c in range(CHUNKS)]
        for c in list(range(1, CHUNKS)) + [0]:
            jobs += [(c, 1, start) for start in range(0, rows - 2 * edge, edge)]
        for number, (c, kind, start) in enumerate(jobs):
            if (c, kind, start) == (0, 1, 0):
                fetch.wait()
            ref = away if (c, kind) == (0, 1) else pieces[2 * c + kind]
            target = start + edge if kind else (rows - edge if start else 0)
            box = (pl.ds(target, edge), pl.ds(c * part, part))
            scaled[box] = ref[start : start + edge, :] * inverse[:, c * part : (c + 1) * part]
            copies.append(pltpu.make_async_copy(scaled.at[box], out_ref.at[box], stored.at[number]))
            copies[-1].start()
        total = jnp.sum(jnp.sum(here_ref[...], axis=0), axis=1, keepdims=True)
        overall_ref[...] = jnp.sqrt(total / (total_rows * across * width) + EPS)
        for copy in copies:
            copy.wait()

    args, specs = [place], [scalar()]
    hbm = pl.BlockSpec(memory_space=pltpu.HBM)
    for c, (outer, inner) in enumerate(state):
        args += [outer, inner if c else in_hbm(inner)]
        specs += [whole(), whole() if c else hbm]
    return call(
        kernel,
        (pltpu.HBM((rows, width), jnp.float32), f32(ITERS + 1, width), f32(1, 1)), specs + [whole(), whole()],
        (hbm, whole(), whole()), rows * width, args + [gathered, known],
        scratch=[
            pltpu.VMEM((rows - 2 * edge, part), jnp.float32),
            pltpu.VMEM((rows, width), jnp.float32),
            pltpu.VMEM((1, width), jnp.float32),
            pltpu.SemaphoreType.DMA((1,)),
            pltpu.SemaphoreType.DMA((CHUNKS * rows // edge,)),
        ],
    )


def swaps(count):
    core = [(i, i ^ 1) for i in range(count) if (i ^ 1) < count]
    cross = []
    for i in range(1, count - 1, 2):
        cross += [(i, i + 1), (i + 1, i)]
    return core, cross


def shards(band_blocks, precond_blocks, right_side):
    nb, br, _ = precond_blocks.shape
    width = right_side.shape[1]
    part = width // CHUNKS
    count = lax.axis_size("rows")
    across = lax.axis_size("rhs")
    core_pairs, cross_pairs = swaps(count)
    odd = (lax.axis_index("rows") % 2).astype(jnp.int32)[None]

    def exchange(cross_send, core_send):
        cross = lax.ppermute(cross_send, "rows", cross_pairs)
        return cross, lax.ppermute(core_send, "rows", core_pairs)

    place = lax.axis_index("rhs").astype(jnp.int32)[None]
    step, halo = [], []
    after = first_edges(right_side, precond_blocks, odd, True, 0, part, None)
    sends = [after, *other_edges(right_side, precond_blocks, odd, part, after)]
    after = sends[-1]
    for c in range(CHUNKS):
        step.append(sends[2 * c : 2 * c + 2])
        halo.append(exchange(*step[c]))
    band = prepare(band_blocks)
    precond = prepare(precond_blocks)
    outer, inner, total = [None] * CHUNKS, [None] * CHUNKS, [None] * CHUNKS
    sums = [[None] * CHUNKS for _ in range(ITERS)]
    latest = [after]

    def run_bulk(sweep, c):
        if sweep < 0:
            residual, edge_step = (right_side,), (odd, *step[c])
        else:
            residual, edge_step = (outer[c], inner[c]), (step[c],)
        done = bulk(residual, edge_step, total[c], band, precond, nb, br, part, c, latest[0])
        outer[c], inner[c], total[c] = done[:3]
        if sweep >= 0:
            sums[sweep][c] = done[3]
        latest[0] = outer[c]

    def run_edges(c):
        outer[c], step[c], cross_send, core_send = edges(
            outer[c], *halo[c], band, precond, odd, nb, br, part, latest[0]
        )
        halo[c] = exchange(cross_send, core_send)
        latest[0] = outer[c]

    for sweep in range(ITERS):
        for c in range(CHUNKS):
            run_bulk(sweep - 1, c)
            run_edges(c)
    for c in range(CHUNKS):
        run_bulk(ITERS - 1, c)
    known = [value for row in sums for value in row]
    local = []
    for c in range(CHUNKS):
        final = c == CHUNKS - 1
        if final:
            known = jnp.concatenate(known + local, axis=1)
            hops = [1 << k for k in range((count - 1).bit_length())]
            for hop in hops[:1] + hops[2:] + hops[1:2]:
                latest[0] = known
                known = known + lax.ppermute(known, "rows", [(i, i ^ hop) for i in range(count)])
        done = edges_last(
            outer[c], inner[c], *halo[c], band, odd, nb, br, part, latest[0],
            None if final else total, jnp.concatenate(local, axis=1) if final else None, count * across,
        )
        outer[c], latest[0] = done[0], done[1]
        if final:
            message = done[1]
        else:
            local.append(done[1])
            answer = done[2]
    gathered = lax.all_to_all(message, ("rows", "rhs"), 0, 0, tiled=True)
    scaled, history, overall = scale_out(
        list(zip(outer, inner)), gathered, known, place, count, across, nb, br, width
    )
    return (answer, scaled, history, overall.reshape(()))


def solution(mesh):
    in_specs = (P("rows", None, None), P("rows", None, None), P("rows", "rhs"))
    out_specs = (P("rows", "rhs"), P("rows", "rhs"), P(None, "rhs"), P())

    return jax.shard_map(shards, mesh=mesh, in_specs=in_specs, out_specs=out_specs, check_vma=False)
```
